32 devices in a mesh: tm: 8 (over z, x), tile: 4 (over y, core).
Axes of the slice: x: 2, y: 2, z: 4, core: 2. Of those that a mesh axis runs over, the one named last changes fastest.
Arguments:
- returns: float32 [2048, 2048], P('tm', 'tile'), may hold values from -6 to 6
- decay_rates: float32 [2048], replicated, may hold values from 9.765625e-05 to 0.015625, as said below
Outputs:
- covariance: float32 [8, 2048, 2048], P('tm', 'tile')
The draws below stay inside these ranges and needn't reach their ends.
Inputs may be any that keep to these rules, and one draw needn't show every extreme that they name: `decay_rates`: every rate is positive.
All inputs are finite; a program needn't handle non-finite values.
Results may differ from the reference program's by a relative error of at most 0.0039.
Values may be sent and summed in bfloat16 or wider, within the bound.
A program may use at most 128 MiB of HBM per device.

```python
import math
import jax
import jax.numpy as jnp
from jax import lax

ASSETS = 2048
SEG = 256
SEGMENTS = 8
DAYS = 2048
N_TM = 8


def draw_decay_rates(key, part):
    pick_key, slow_key, fast_key = jax.random.split(jax.random.fold_in(key, 11), 3)
    pick = jax.random.uniform(pick_key, (ASSETS,), dtype=jnp.float32)
    slow_u = jax.random.uniform(slow_key, (ASSETS,), dtype=jnp.float32)
    fast_u = jax.random.uniform(fast_key, (ASSETS,), dtype=jnp.float32)
    slow = 0.2 / DAYS * jnp.exp(slow_u * math.log(5.0))
    fast = 1.2 / SEG * jnp.exp(fast_u * math.log(4.0 / 1.2))
    share = 0.25
    rate = jnp.where(pick < share, fast, slow)
    return rate.astype(jnp.float32)


def draw_returns(key, part):
    phase_key, jitter_key, base_key = jax.random.split(jax.random.fold_in(key, 23), 3)
    phase = jax.random.randint(phase_key, (), 0, 2)
    seg_index = jnp.arange(SEGMENTS, dtype=jnp.int32)
    jitter = jnp.exp(jax.random.uniform(jitter_key, (SEGMENTS,), dtype=jnp.float32, minval=-0.2, maxval=0.2))
    level = jnp.where((seg_index + phase) % 2 == 0, 1.0, 0.2) * jitter
    base = jnp.clip(jax.random.normal(base_key, (DAYS, ASSETS), dtype=jnp.float32), -4.8, 4.8)
    values = base.reshape(SEGMENTS, SEG, ASSETS) * level[:, None, None]
    values = jnp.clip(values, -6.0, 6.0).reshape(DAYS, ASSETS)
    return values.astype(jnp.float32)


def setup_inputs(seed: int = 0) -> dict:
    keys = jax.random.split(jax.random.key(seed), 3)
    returns = draw_returns(jax.random.fold_in(keys[2], 71), 0)
    decay_rates = draw_decay_rates(jax.random.fold_in(keys[2], 71), 0)
    return dict(returns=returns, decay_rates=decay_rates)


def reference(returns, decay_rates):
    segments_in = returns.reshape(N_TM, SEG, ASSETS)
    days_left = (SEG - 1 - jnp.arange(SEG)).astype(jnp.float32)
    scaling = jnp.exp(-decay_rates[None, :] * days_left[:, None])
    pair_rate = decay_rates[:, None] + decay_rates[None, :]
    seg_decay = jnp.exp(-pair_rate * SEG)
    geometric = jnp.expm1(-pair_rate)

    def advance(running, payload):
        seg_rows, seg_index = payload
        scaled = (seg_rows * scaling).astype(jnp.bfloat16).astype(jnp.float32)
        gram_all = jnp.dot(scaled.T, scaled, preferred_element_type=jnp.float32, precision=lax.Precision.HIGHEST)
        running = running * seg_decay + gram_all
        elapsed = (seg_index + 1).astype(jnp.float32) * SEG
        weights = jnp.expm1(-pair_rate * elapsed) / geometric
        return running, running / weights

    start_sum = jnp.zeros((ASSETS, ASSETS), jnp.float32)
    _, covariance = lax.scan(advance, start_sum, (segments_in, jnp.arange(N_TM, dtype=jnp.int32)))
    return covariance
```

```python
import functools

import jax
import jax.numpy as jnp
from jax import lax
from jax.experimental import pallas as pl
from jax.experimental.pallas import tpu as pltpu
from jax.sharding import PartitionSpec as P

MESH = pl.DeviceIdType.MESH
F32 = jnp.float32
CORES = 2


def expm1_neg(x):
    near = jnp.maximum(x, -0.5)
    series = jnp.ones_like(x)
    for n in range(9, 1, -1):
        series = 1.0 + near * (1.0 / n) * series
    return jnp.where(x > -0.5, near * series, jnp.exp(x) - 1.0)


def gather_kernel(periods, tiles, returns_ref, rates_ref, out_ref, buf, cols, ssem, rsem):
    seg_days, block = returns_ref.shape
    width = tiles // CORES
    planes = periods // width
    half = seg_days // 2
    s = lax.axis_index("tm")
    t = lax.axis_index("tile")
    z, x = s // width, s % width
    y, c = t // CORES, t % CORES
    yt = (1 - y) * CORES + c
    pt = y * CORES + (1 - c)
    pyt = (1 - y) * CORES + (1 - c)
    sx = z * width + (1 - x)
    x_dev, y_dev, p_dev = (sx, t), (s, yt), (s, pt)
    up_dev, down_dev = (s + width, t), (s - width, t)
    has_up, has_down = z < planes - 1, z > 0

    barrier = pltpu.get_barrier_semaphore()
    for dev in (x_dev, y_dev, p_dev):
        pl.semaphore_signal(barrier, inc=1, device_id=dev, device_id_type=MESH)

    @pl.when(has_up)
    def _():
        pl.semaphore_signal(barrier, inc=1, device_id=up_dev, device_id_type=MESH)

    @pl.when(has_down)
    def _():
        pl.semaphore_signal(barrier, inc=1, device_id=down_dev, device_id_type=MESH)

    own = pl.ds(pl.multiple_of(t * block, block), block)
    own_rates = rates_ref[:, own]
    days_left = (seg_days - 1 - lax.broadcasted_iota(jnp.int32, (seg_days, block), 0)).astype(F32)
    buf[s, t] = (returns_ref[...] * jnp.exp(-own_rates * days_left)).astype(jnp.bfloat16)
    cols[...] = jnp.transpose(jnp.broadcast_to(own_rates, (128, block)))

    pl.semaphore_wait(barrier, 3 + has_up.astype(jnp.int32) + has_down.astype(jnp.int32))

    sent = []

    def copy(sp, tp, h, dev, sem):
        part = buf.at[sp, tp, pl.ds(h * half, half)]
        return pltpu.make_async_remote_copy(
            part, part, sem, rsem.at[sp, tp, h], device_id=dev, device_id_type=MESH
        )

    def arrived(sp, tp, h):
        copy(sp, tp, h, p_dev, ssem.at[0, 0]).wait_recv()

    def plane(d):
        exists = z >= d
        sa = (z - d) * width + x
        sb = (z - d) * width + (1 - x)
        x_takes = exists & (sa <= sx)
        x_gives = exists & (sb <= s)
        count = [0]

        def send(cond, sp, tp, h, dev):
            sem = ssem.at[d, count[0]]
            count[0] += 1
            sent.append((cond, sp, tp, h, dev, sem))

            @pl.when(cond)
            def _():
                copy(sp, tp, h, dev, sem).start()

        def wait(cond, sp, tp, h):
            @pl.when(cond)
            def _():
                arrived(sp, tp, h)

        def column():
            for h in (0, 1):
                if d:
                    wait(exists, sa, t, h)
                send(exists & has_up, sa, t, h, up_dev)
                send(x_takes, sa, t, h, x_dev)
                send(exists, sa, t, h, y_dev)
                send(exists, sa, t, h, p_dev)

        def across():
            for h in (0, 1):
                wait(x_gives, sb, t, h)
                if h == 0:
                    send(x_gives, sb, t, h, y_dev)
                send(x_gives, sb, t, h, p_dev)
                wait(exists, sa, yt, h)
                if h == 1:
                    send(x_takes, sa, yt, h, x_dev)
                send(exists, sa, yt, h, p_dev)
            for h in (0, 1):
                wait(x_gives, sb, yt, h)
                send(x_gives, sb, yt, h, p_dev)

        def partner():
            for h in (0, 1):
                wait(exists, sa, pt, h)
                wait(exists, sa, pyt, h)
                wait(x_gives, sb, pt, h)
                wait(x_gives, sb, pyt, h)

        def compute():
            for cond, sp in ((exists, sa), (x_gives, sb)):

                @pl.when(cond)
                def _(sp=sp):
                    lag = ((s - sp) * seg_days).astype(F32)
                    lhs = buf[sp, t]
                    col = jnp.exp(-cols[...] * lag)

                    def step(tp, _):
                        at = pl.ds(pl.multiple_of(tp * block, block), block)
                        gram = lax.dot_general(
                            lhs, buf[sp, tp], (((0,), (0,)), ((), ())), preferred_element_type=F32
                        )
                        row = jnp.exp(-rates_ref[:, at] * lag)
                        for j in range(block // 128):
                            lane = slice(j * 128, (j + 1) * 128)
                            here = pl.ds(pl.multiple_of(tp * block + j * 128, 128), 128)
                            term = gram[:, lane] * (col * row[:, lane])
                            if d == 0 and sp is sa:
                                out_ref[:, here] = term
                            else:
                                out_ref[:, here] += term
                        return 0

                    lax.fori_loop(0, tiles, step, 0)

        return column, across, partner, compute

    steps = [plane(d) for d in range(planes)]
    steps[0][0]()
    for d in range(planes):
        if d + 1 < planes:
            steps[d + 1][0]()
        for stage in steps[d][1:]:
            stage()

    elapsed = ((s + 1) * seg_days).astype(F32)
    u1, un = expm1_neg(-cols[...]), expm1_neg(-cols[...] * elapsed)

    def finish(j, _):
        at = pl.ds(pl.multiple_of(j * 128, 128), 128)
        rates = rates_ref[:, at]
        v1, vn = expm1_neg(-rates), expm1_neg(-rates * elapsed)
        out_ref[:, at] = out_ref[:, at] * ((u1 + v1 + u1 * v1) / (un + vn + un * vn))
        return 0

    lax.fori_loop(0, out_ref.shape[1] // 128, finish, 0)

    for cond, sp, tp, h, dev, sem in sent:

        @pl.when(cond)
        def _(sp=sp, tp=tp, h=h, dev=dev, sem=sem):
            copy(sp, tp, h, dev, sem).wait_send()


def by_gather(returns, decay_rates):
    seg_days, block = returns.shape
    periods, tiles = lax.axis_size("tm"), lax.axis_size("tile")
    assets = decay_rates.shape[0]
    planes = periods // (tiles // CORES)
    vmem = pl.BlockSpec(memory_space=pltpu.VMEM)
    return pl.pallas_call(
        functools.partial(gather_kernel, periods, tiles),
        out_shape=jax.ShapeDtypeStruct((block, assets), F32),
        in_specs=[vmem, vmem],
        out_specs=vmem,
        scratch_shapes=[
            pltpu.VMEM((periods, tiles, seg_days, block), jnp.bfloat16),
            pltpu.VMEM((block, 128), F32),
            pltpu.SemaphoreType.DMA((planes, 18)),
            pltpu.SemaphoreType.DMA((periods, tiles, 2)),
        ],
        compiler_params=pltpu.CompilerParams(
            collective_id=0, has_side_effects=True, vmem_limit_bytes=40 * 2**20
        ),
        name="gather_sums",
    )(returns, decay_rates[None])[None]


def by_exchange(returns, decay_rates):
    seg_days, col_block = returns.shape
    tile_at = lax.axis_index("tile")
    seg_at = lax.axis_index("tm")
    days_left = (seg_days - 1 - jnp.arange(seg_days)).astype(jnp.float32)
    own_rates = lax.dynamic_slice_in_dim(decay_rates, tile_at * col_block, col_block)
    scaled = (returns * jnp.exp(-own_rates[None, :] * days_left[:, None])).astype(jnp.bfloat16)
    gram_rows = lax.dot_general(
        scaled,
        lax.all_gather(scaled, "tile", axis=1, tiled=True),
        (((0,), (0,)), ((), ())),
        preferred_element_type=jnp.float32,
    )
    pair_rate = own_rates[:, None] + decay_rates[None, :]
    seg_decay = jnp.exp(-pair_rate * seg_days)
    periods = lax.axis_size("tm")
    row_piece = col_block // periods
    spread = lax.all_to_all(gram_rows[None], "tm", split_axis=1, concat_axis=0, tiled=True)
    row_rates = lax.dynamic_slice_in_dim(
        decay_rates, tile_at * col_block + seg_at * row_piece, row_piece
    )
    row_decay = jnp.exp(-(row_rates[:, None] + decay_rates[None, :]) * seg_days)

    def advance(running, segment_term):
        return (running * row_decay + segment_term, running)

    _, prefix = lax.scan(advance, jnp.zeros_like(spread[0]), spread)
    carried = lax.all_to_all(prefix, "tm", split_axis=0, concat_axis=1, tiled=True)[0]
    running = carried * seg_decay + gram_rows
    elapsed = (seg_at + 1).astype(jnp.float32) * seg_days
    weights = jnp.expm1(-pair_rate * elapsed) / jnp.expm1(-pair_rate)
    return (running / weights)[None]


def solution(mesh):
    placed = (P("tm", "tile"), P())
    pairs = mesh.shape["tile"] == 2 * CORES
    per_device = by_gather if pairs else by_exchange
    return jax.shard_map(
        per_device, mesh=mesh, in_specs=placed, out_specs=P("tm", "tile", None), check_vma=False
    )
```

```python
import functools

import jax
import jax.numpy as jnp
from jax import lax
from jax.experimental import pallas as pl
from jax.experimental.pallas import tpu as pltpu
from jax.sharding import PartitionSpec as P

MESH = pl.DeviceIdType.MESH
F32 = jnp.float32
CORES = 2


def expm1_neg(x):
    near = jnp.maximum(x, -0.5)
    series = jnp.ones_like(x)
    for n in range(9, 1, -1):
        series = 1.0 + near * (1.0 / n) * series
    return jnp.where(x > -0.5, near * series, jnp.exp(x) - 1.0)


def gather_kernel(
    periods, tiles, returns_ref, rates_ref, out_ref, buf, left, cols, ssem, rsem
):
    seg_days, block = returns_ref.shape
    width = tiles // CORES
    planes = periods // width
    half = seg_days // 2
    s = lax.axis_index("tm")
    t = lax.axis_index("tile")
    z, x = s // width, s % width
    y, c = t // CORES, t % CORES
    yt = (1 - y) * CORES + c
    pt = y * CORES + (1 - c)
    pyt = (1 - y) * CORES + (1 - c)
    sx = z * width + (1 - x)
    x_dev, y_dev, p_dev = (sx, t), (s, yt), (s, pt)
    up_dev, down_dev = (s + width, t), (s - width, t)
    has_up, has_down = z < planes - 1, z > 0

    barrier = pltpu.get_barrier_semaphore()
    for dev in (x_dev, y_dev, p_dev):
        pl.semaphore_signal(barrier, inc=1, device_id=dev, device_id_type=MESH)

    @pl.when(has_up)
    def _():
        pl.semaphore_signal(barrier, inc=1, device_id=up_dev, device_id_type=MESH)

    @pl.when(has_down)
    def _():
        pl.semaphore_signal(barrier, inc=1, device_id=down_dev, device_id_type=MESH)

    out_ref[...] = jnp.zeros_like(out_ref)
    own = pl.ds(pl.multiple_of(t * block, block), block)
    own_rates = rates_ref[:, own]
    days_left = (seg_days - 1 - lax.broadcasted_iota(jnp.int32, (seg_days, block), 0)).astype(F32)
    buf[s, t] = (returns_ref[...] * jnp.exp(-own_rates * days_left)).astype(jnp.bfloat16)
    cols[...] = jnp.transpose(jnp.broadcast_to(own_rates, (128, block)))

    pl.semaphore_wait(barrier, 3 + has_up.astype(jnp.int32) + has_down.astype(jnp.int32))

    sent = []

    def copy(sp, tp, h, dev, sem):
        part = buf.at[sp, tp, pl.ds(h * half, half)]
        return pltpu.make_async_remote_copy(
            part, part, sem, rsem.at[sp, tp, h], device_id=dev, device_id_type=MESH
        )

    def arrived(sp, tp, h):
        copy(sp, tp, h, p_dev, ssem.at[0, 0]).wait_recv()

    def plane(d):
        exists = z >= d
        sa = (z - d) * width + x
        sb = (z - d) * width + (1 - x)
        x_takes = exists & (sa <= sx)
        x_gives = exists & (sb <= s)
        count = [0]

        def send(cond, sp, tp, h, dev):
            sem = ssem.at[d, count[0]]
            count[0] += 1
            sent.append((cond, sp, tp, h, dev, sem))

            @pl.when(cond)
            def _():
                copy(sp, tp, h, dev, sem).start()

        def wait(cond, sp, tp, h):
            @pl.when(cond)
            def _():
                arrived(sp, tp, h)

        def column(h):
            if d:
                wait(exists, sa, t, h)
            send(exists & has_up, sa, t, h, up_dev)
            send(x_takes, sa, t, h, x_dev)
            send(exists, sa, t, h, y_dev)
            send(exists, sa, t, h, p_dev)

        def across(h):
            wait(x_gives, sb, t, h)
            if h == 0:
                send(x_gives, sb, t, h, y_dev)
            send(x_gives, sb, t, h, p_dev)
            wait(exists, sa, yt, h)
            if h == 1:
                send(x_takes, sa, yt, h, x_dev)
            send(exists, sa, yt, h, p_dev)

        def corner():
            for h in (0, 1):
                wait(x_gives, sb, yt, h)
                send(x_gives, sb, yt, h, p_dev)

        def transpose(sp):
            left[sp] = jnp.transpose(buf[sp, t])

        def product(sp, tp):
            lag = ((s - sp) * seg_days).astype(F32)
            gram = jnp.dot(left[sp], buf[sp, tp], preferred_element_type=F32)
            at = pl.ds(pl.multiple_of(tp * block, block), block)
            col, row = jnp.exp(-cols[...] * lag), jnp.exp(-rates_ref[:, at] * lag)
            for j in range(block // 128):
                lane = slice(j * 128, (j + 1) * 128)
                here = pl.ds(pl.multiple_of(tp * block + j * 128, 128), 128)
                out_ref[:, here] += gram[:, lane] * (col * row[:, lane])

        def products(first, last, which):
            def step(i, _):
                product(*which(i))
                return 0

            lax.fori_loop(first, last, step, 0)

        def column_products():
            @pl.when(exists)
            def _():
                for h in (0, 1):
                    arrived(sa, pt, h)
                transpose(sa)
                products(0, 2, lambda i: (sa, y * CORES + i))

        def across_products():
            for h in (0, 1):
                wait(x_gives, sb, pt, h)
                wait(exists, sa, pyt, h)

            @pl.when(x_gives)
            def _():
                transpose(sb)

            @pl.when(exists)
            def _():
                products(
                    jnp.where(x_gives, 0, 2),
                    4,
                    lambda i: (
                        jnp.where(i < 2, sb, sa),
                        jnp.where(i < 2, y * CORES + i, (1 - y) * CORES + i - 2),
                    ),
                )

        def corner_products():
            @pl.when(x_gives)
            def _():
                for h in (0, 1):
                    arrived(sb, pyt, h)
                products(0, 2, lambda i: (sb, (1 - y) * CORES + i))

        return column, across, corner, column_products, across_products, corner_products

    column, across, corner, column_products, across_products, corner_products = zip(
        *[plane(d) for d in range(planes)]
    )

    elapsed = ((s + 1) * seg_days).astype(F32)

    def finish(first):
        u1, un = expm1_neg(-cols[...]), expm1_neg(-cols[...] * elapsed)

        def step(j, _):
            at = pl.ds(pl.multiple_of(first * block + j * 128, 128), 128)
            rates = rates_ref[:, at]
            v1, vn = expm1_neg(-rates), expm1_neg(-rates * elapsed)
            out_ref[:, at] = out_ref[:, at] * ((u1 + v1 + u1 * v1) / (un + vn + un * vn))
            return 0

        lax.fori_loop(0, CORES * block // 128, step, 0)

    column[0](0)
    column[0](1)
    column_products[0]()
    for d in range(planes):
        more = d + 1 < planes
        if more:
            column[d + 1](0)
        if d:
            corner[d - 1]()
        across[d](0)
        if more:
            column[d + 1](1)
        across[d](1)
        if d:
            corner_products[d - 1]()
        across_products[d]()
        if more:
            column_products[d + 1]()
    finish(y * CORES)
    corner[-1]()
    corner_products[-1]()
    finish((1 - y) * CORES)

    for cond, sp, tp, h, dev, sem in sent:

        @pl.when(cond)
        def _(sp=sp, tp=tp, h=h, dev=dev, sem=sem):
            copy(sp, tp, h, dev, sem).wait_send()


def by_gather(returns, decay_rates):
    seg_days, block = returns.shape
    periods, tiles = lax.axis_size("tm"), lax.axis_size("tile")
    assets = decay_rates.shape[0]
    planes = periods // (tiles // CORES)
    vmem = pl.BlockSpec(memory_space=pltpu.VMEM)
    return pl.pallas_call(
        functools.partial(gather_kernel, periods, tiles),
        out_shape=jax.ShapeDtypeStruct((block, assets), F32),
        in_specs=[vmem, vmem],
        out_specs=vmem,
        scratch_shapes=[
            pltpu.VMEM((periods, tiles, seg_days, block), jnp.bfloat16),
            pltpu.VMEM((periods, block, seg_days), jnp.bfloat16),
            pltpu.VMEM((block, 128), F32),
            pltpu.SemaphoreType.DMA((planes, 18)),
            pltpu.SemaphoreType.DMA((periods, tiles, 2)),
        ],
        compiler_params=pltpu.CompilerParams(
            collective_id=0, has_side_effects=True, vmem_limit_bytes=40 * 2**20
        ),
        name="gather_sums",
    )(returns, decay_rates[None])[None]


def by_exchange(returns, decay_rates):
    seg_days, col_block = returns.shape
    tile_at = lax.axis_index("tile")
    seg_at = lax.axis_index("tm")
    days_left = (seg_days - 1 - jnp.arange(seg_days)).astype(jnp.float32)
    own_rates = lax.dynamic_slice_in_dim(decay_rates, tile_at * col_block, col_block)
    scaled = (returns * jnp.exp(-own_rates[None, :] * days_left[:, None])).astype(jnp.bfloat16)
    gram_rows = lax.dot_general(
        scaled,
        lax.all_gather(scaled, "tile", axis=1, tiled=True),
        (((0,), (0,)), ((), ())),
        preferred_element_type=jnp.float32,
    )
    pair_rate = own_rates[:, None] + decay_rates[None, :]
    seg_decay = jnp.exp(-pair_rate * seg_days)
    periods = lax.axis_size("tm")
    row_piece = col_block // periods
    spread = lax.all_to_all(gram_rows[None], "tm", split_axis=1, concat_axis=0, tiled=True)
    row_rates = lax.dynamic_slice_in_dim(
        decay_rates, tile_at * col_block + seg_at * row_piece, row_piece
    )
    row_decay = jnp.exp(-(row_rates[:, None] + decay_rates[None, :]) * seg_days)

    def advance(running, segment_term):
        return (running * row_decay + segment_term, running)

    _, prefix = lax.scan(advance, jnp.zeros_like(spread[0]), spread)
    carried = lax.all_to_all(prefix, "tm", split_axis=0, concat_axis=1, tiled=True)[0]
    running = carried * seg_decay + gram_rows
    elapsed = (seg_at + 1).astype(jnp.float32) * seg_days
    weights = jnp.expm1(-pair_rate * elapsed) / jnp.expm1(-pair_rate)
    return (running / weights)[None]


def solution(mesh):
    placed = (P("tm", "tile"), P())
    pairs = mesh.shape["tile"] == 2 * CORES
    per_device = by_gather if pairs else by_exchange
    return jax.shard_map(
        per_device, mesh=mesh, in_specs=placed, out_specs=P("tm", "tile", None), check_vma=False
    )
```

```python
import functools

import jax
import jax.numpy as jnp
from jax import lax
from jax.experimental import pallas as pl
from jax.experimental.pallas import tpu as pltpu
from jax.sharding import PartitionSpec as P

MESH = pl.DeviceIdType.MESH
F32 = jnp.float32
CORES = 2


def expm1_neg(x):
    near = jnp.maximum(x, -0.5)
    series = jnp.ones_like(x)
    for n in range(9, 1, -1):
        series = 1.0 + near * (1.0 / n) * series
    return jnp.where(x > -0.5, near * series, jnp.exp(x) - 1.0)


def gather_kernel(
    periods, tiles, returns_ref, rates_ref, out_ref, buf, left, ratio, cols, ssem, rsem
):
    seg_days, block = returns_ref.shape
    width = tiles // CORES
    planes = periods // width
    half = seg_days // 2
    s = lax.axis_index("tm")
    t = lax.axis_index("tile")
    z, x = s // width, s % width
    y, c = t // CORES, t % CORES
    yt = (1 - y) * CORES + c
    pt = y * CORES + (1 - c)
    pyt = (1 - y) * CORES + (1 - c)
    sx = z * width + (1 - x)
    x_dev, y_dev, p_dev = (sx, t), (s, yt), (s, pt)
    up_dev, down_dev = (s + width, t), (s - width, t)
    has_up, has_down = z < planes - 1, z > 0
    up_half = 1 - c

    barrier = pltpu.get_barrier_semaphore()
    for dev in (x_dev, y_dev, p_dev):
        pl.semaphore_signal(barrier, inc=1, device_id=dev, device_id_type=MESH)

    @pl.when(has_up)
    def _():
        pl.semaphore_signal(barrier, inc=1, device_id=up_dev, device_id_type=MESH)

    @pl.when(has_down)
    def _():
        pl.semaphore_signal(barrier, inc=1, device_id=down_dev, device_id_type=MESH)

    out_ref[...] = jnp.zeros_like(out_ref)
    own = pl.ds(pl.multiple_of(t * block, block), block)
    own_rates = rates_ref[:, own]
    days_left = (seg_days - 1 - lax.broadcasted_iota(jnp.int32, (seg_days, block), 0)).astype(F32)
    buf[s, t] = (returns_ref[...] * jnp.exp(-own_rates * days_left)).astype(jnp.bfloat16)
    cols[...] = jnp.transpose(jnp.broadcast_to(own_rates, (128, block)))

    pl.semaphore_wait(barrier, 3 + has_up.astype(jnp.int32) + has_down.astype(jnp.int32))

    sent = []

    def copy(sp, tp, h, dev, sem):
        part = buf.at[sp, tp, pl.ds(pl.multiple_of(h * half, half), half)]
        return pltpu.make_async_remote_copy(
            part, part, sem, rsem.at[sp, tp, h], device_id=dev, device_id_type=MESH
        )

    def arrived(sp, tp, h):
        copy(sp, tp, h, p_dev, ssem.at[0, 0]).wait_recv()

    def plane(d):
        exists = z >= d
        sa = (z - d) * width + x
        sb = (z - d) * width + (1 - x)
        x_takes = exists & (sa <= sx)
        x_gives = exists & (sb <= s)
        count = [0]

        def send(cond, sp, tp, h, dev):
            sem = ssem.at[d, count[0]]
            count[0] += 1
            sent.append((cond, sp, tp, h, dev, sem))

            @pl.when(cond)
            def _():
                copy(sp, tp, h, dev, sem).start()

        def wait(cond, sp, tp, h):
            @pl.when(cond)
            def _():
                arrived(sp, tp, h)

        def column(h):
            if d:
                wait(exists, sa, t, h)
            send(exists & has_up, sa, t, h, up_dev)
            send(x_takes, sa, t, h, x_dev)
            send(exists, sa, t, h, y_dev)
            send(exists, sa, t, h, p_dev)

        def across(h):
            wait(x_gives, sb, t, h)
            if h == 0:
                send(x_gives & (c == 0) if d else x_gives, sb, t, h, y_dev)
            send(x_gives, sb, t, h, p_dev)
            wait(exists, sa, yt, h)
            if h == 1:
                send(x_takes & (c == 1) if d else x_takes, sa, yt, h, x_dev)
            if d == 0:
                send((x == 1) & has_up & (up_half == h), sa, yt, h, x_dev)
            send(exists, sa, yt, h, p_dev)

        def corner():
            wait(exists & has_up | x_gives, sb, yt, up_half)
            send(exists & has_up, sb, yt, up_half, up_dev)
            send(x_gives, sb, yt, up_half, p_dev)
            wait(x_gives, sb, yt, 1 - up_half)
            send(x_gives, sb, yt, 1 - up_half, p_dev)

        def transpose(sp):
            left[sp] = jnp.transpose(buf[sp, t])

        def product(sp, tp):
            lag = ((s - sp) * seg_days).astype(F32)
            gram = jnp.dot(left[sp], buf[sp, tp], preferred_element_type=F32)
            at = pl.ds(pl.multiple_of(tp * block, block), block)
            col, row = jnp.exp(-cols[...] * lag), jnp.exp(-rates_ref[:, at] * lag)
            for j in range(block // 128):
                lane = slice(j * 128, (j + 1) * 128)
                here = pl.ds(pl.multiple_of(tp * block + j * 128, 128), 128)
                out_ref[:, here] += gram[:, lane] * (col * row[:, lane])

        def products(first, last, which):
            def step(i, _):
                product(*which(i))
                return 0

            lax.fori_loop(first, last, step, 0)

        def column_products():
            @pl.when(exists)
            def _():
                for h in (0, 1):
                    arrived(sa, pt, h)
                transpose(sa)
                products(0, 2, lambda i: (sa, y * CORES + i))

        def across_products():
            for h in (0, 1):
                wait(x_gives, sb, pt, h)
                wait(exists, sa, pyt, h)

            @pl.when(x_gives)
            def _():
                transpose(sb)

            @pl.when(exists)
            def _():
                products(
                    jnp.where(x_gives, 0, 2),
                    4,
                    lambda i: (
                        jnp.where(i < 2, sb, sa),
                        jnp.where(i < 2, y * CORES + i, (1 - y) * CORES + i - 2),
                    ),
                )

        def corner_products():
            @pl.when(x_gives)
            def _():
                for h in (0, 1):
                    arrived(sb, pyt, h)
                products(0, 2, lambda i: (sb, (1 - y) * CORES + i))

        return column, across, corner, column_products, across_products, corner_products

    column, across, corner, column_products, across_products, corner_products = zip(
        *[plane(d) for d in range(planes)]
    )

    elapsed = ((s + 1) * seg_days).astype(F32)

    def weigh(first):
        u1, un = expm1_neg(-cols[...]), expm1_neg(-cols[...] * elapsed)

        def step(j, _):
            at = pl.ds(pl.multiple_of(first * block + j * 128, 128), 128)
            rates = rates_ref[:, at]
            v1, vn = expm1_neg(-rates), expm1_neg(-rates * elapsed)
            ratio[:, at] = (u1 + v1 + u1 * v1) / (un + vn + un * vn)
            return 0

        lax.fori_loop(0, CORES * block // 128, step, 0)

    def finish(first):
        at = pl.ds(pl.multiple_of(first * block, block), CORES * block)
        out_ref[:, at] = out_ref[:, at] * ratio[:, at]

    column[0](0)
    column[0](1)
    column_products[0]()
    weigh(y * CORES)
    for d in range(planes):
        more = d + 1 < planes
        if more:
            column[d + 1](0)
        if d:
            corner[d - 1]()
        across[d](0)
        if more:
            column[d + 1](1)
        across[d](1)
        if d:
            corner_products[d - 1]()
        across_products[d]()
        if d == 1:
            weigh((1 - y) * CORES)
        if more:
            column_products[d + 1]()
    finish(y * CORES)
    corner[-1]()
    corner_products[-1]()
    finish((1 - y) * CORES)

    for cond, sp, tp, h, dev, sem in sent:

        @pl.when(cond)
        def _(sp=sp, tp=tp, h=h, dev=dev, sem=sem):
            copy(sp, tp, h, dev, sem).wait_send()


def by_gather(returns, decay_rates):
    seg_days, block = returns.shape
    periods, tiles = lax.axis_size("tm"), lax.axis_size("tile")
    assets = decay_rates.shape[0]
    planes = periods // (tiles // CORES)
    vmem = pl.BlockSpec(memory_space=pltpu.VMEM)
    return pl.pallas_call(
        functools.partial(gather_kernel, periods, tiles),
        out_shape=jax.ShapeDtypeStruct((block, assets), F32),
        in_specs=[vmem, vmem],
        out_specs=vmem,
        scratch_shapes=[
            pltpu.VMEM((periods, tiles, seg_days, block), jnp.bfloat16),
            pltpu.VMEM((periods, block, seg_days), jnp.bfloat16),
            pltpu.VMEM((block, assets), F32),
            pltpu.VMEM((block, 128), F32),
            pltpu.SemaphoreType.DMA((planes, 20)),
            pltpu.SemaphoreType.DMA((periods, tiles, 2)),
        ],
        compiler_params=pltpu.CompilerParams(
            collective_id=0, has_side_effects=True, vmem_limit_bytes=40 * 2**20
        ),
        name="gather_sums",
    )(returns, decay_rates[None])[None]


def by_exchange(returns, decay_rates):
    seg_days, col_block = returns.shape
    tile_at = lax.axis_index("tile")
    seg_at = lax.axis_index("tm")
    days_left = (seg_days - 1 - jnp.arange(seg_days)).astype(jnp.float32)
    own_rates = lax.dynamic_slice_in_dim(decay_rates, tile_at * col_block, col_block)
    scaled = (returns * jnp.exp(-own_rates[None, :] * days_left[:, None])).astype(jnp.bfloat16)
    gram_rows = lax.dot_general(
        scaled,
        lax.all_gather(scaled, "tile", axis=1, tiled=True),
        (((0,), (0,)), ((), ())),
        preferred_element_type=jnp.float32,
    )
    pair_rate = own_rates[:, None] + decay_rates[None, :]
    seg_decay = jnp.exp(-pair_rate * seg_days)
    periods = lax.axis_size("tm")
    row_piece = col_block // periods
    spread = lax.all_to_all(gram_rows[None], "tm", split_axis=1, concat_axis=0, tiled=True)
    row_rates = lax.dynamic_slice_in_dim(
        decay_rates, tile_at * col_block + seg_at * row_piece, row_piece
    )
    row_decay = jnp.exp(-(row_rates[:, None] + decay_rates[None, :]) * seg_days)

    def advance(running, segment_term):
        return (running * row_decay + segment_term, running)

    _, prefix = lax.scan(advance, jnp.zeros_like(spread[0]), spread)
    carried = lax.all_to_all(prefix, "tm", split_axis=0, concat_axis=1, tiled=True)[0]
    running = carried * seg_decay + gram_rows
    elapsed = (seg_at + 1).astype(jnp.float32) * seg_days
    weights = jnp.expm1(-pair_rate * elapsed) / jnp.expm1(-pair_rate)
    return (running / weights)[None]


def solution(mesh):
    placed = (P("tm", "tile"), P())
    pairs = mesh.shape["tile"] == 2 * CORES
    per_device = by_gather if pairs else by_exchange
    return jax.shard_map(
        per_device, mesh=mesh, in_specs=placed, out_specs=P("tm", "tile", None), check_vma=False
    )
```

```python
import functools

import jax
import jax.numpy as jnp
from jax import lax
from jax.experimental import pallas as pl
from jax.experimental.pallas import tpu as pltpu
from jax.sharding import PartitionSpec as P

MESH = pl.DeviceIdType.MESH
F32 = jnp.float32
CORES = 2


def expm1_neg(x):
    near = jnp.maximum(x, -0.5)
    series = jnp.ones_like(x)
    for n in range(9, 1, -1):
        series = 1.0 + near * (1.0 / n) * series
    return jnp.where(x > -0.5, near * series, jnp.exp(x) - 1.0)


def gather_kernel(
    periods, tiles, returns_ref, rates_ref, out_ref, buf, left, ratio, cols, ssem, rsem
):
    seg_days, block = returns_ref.shape
    width = tiles // CORES
    planes = periods // width
    half = seg_days // 2
    s = lax.axis_index("tm")
    t = lax.axis_index("tile")
    z, x = s // width, s % width
    y, c = t // CORES, t % CORES
    yt = (1 - y) * CORES + c
    pt = y * CORES + (1 - c)
    pyt = (1 - y) * CORES + (1 - c)
    sx = z * width + (1 - x)
    x_dev, y_dev, p_dev = (sx, t), (s, yt), (s, pt)
    up_dev, down_dev = (s + width, t), (s - width, t)
    has_up, has_down = z < planes - 1, z > 0
    up_half = 1

    barrier = pltpu.get_barrier_semaphore()
    for dev in (x_dev, y_dev, p_dev):
        pl.semaphore_signal(barrier, inc=1, device_id=dev, device_id_type=MESH)

    @pl.when(has_up)
    def _():
        pl.semaphore_signal(barrier, inc=1, device_id=up_dev, device_id_type=MESH)

    @pl.when(has_down)
    def _():
        pl.semaphore_signal(barrier, inc=1, device_id=down_dev, device_id_type=MESH)

    out_ref[...] = jnp.zeros_like(out_ref)
    own = pl.ds(pl.multiple_of(t * block, block), block)
    own_rates = rates_ref[:, own]
    days_left = (seg_days - 1 - lax.broadcasted_iota(jnp.int32, (seg_days, block), 0)).astype(F32)
    buf[s, t] = (returns_ref[...] * jnp.exp(-own_rates * days_left)).astype(jnp.bfloat16)
    cols[...] = jnp.transpose(jnp.broadcast_to(own_rates, (128, block)))

    pl.semaphore_wait(barrier, 3 + has_up.astype(jnp.int32) + has_down.astype(jnp.int32))

    sent = []

    def copy(sp, tp, h, dev, sem):
        part = buf.at[sp, tp, pl.ds(pl.multiple_of(h * half, half), half)]
        return pltpu.make_async_remote_copy(
            part, part, sem, rsem.at[sp, tp, h], device_id=dev, device_id_type=MESH
        )

    def arrived(sp, tp, h):
        copy(sp, tp, h, p_dev, ssem.at[0, 0]).wait_recv()

    def plane(d):
        exists = z >= d
        sa = (z - d) * width + x
        sb = (z - d) * width + (1 - x)
        x_takes = exists & (sa <= sx)
        x_gives = exists & (sb <= s)
        count = [0]

        def send(cond, sp, tp, h, dev):
            sem = ssem.at[d, count[0]]
            count[0] += 1
            sent.append((cond, sp, tp, h, dev, sem))

            @pl.when(cond)
            def _():
                copy(sp, tp, h, dev, sem).start()

        def wait(cond, sp, tp, h):
            @pl.when(cond)
            def _():
                arrived(sp, tp, h)

        def column(h):
            if d:
                wait(exists, sa, t, h)
            send(exists & has_up, sa, t, h, up_dev)
            send(x_takes, sa, t, h, x_dev)
            send(exists, sa, t, h, y_dev)
            send(exists, sa, t, h, p_dev)

        def across(h):
            wait(x_gives, sb, t, h)
            if h == 0:
                send(x_gives & (c == 0) if d else x_gives, sb, t, h, y_dev)
            send(x_gives, sb, t, h, p_dev)
            wait(exists, sa, yt, h)
            if d == 0 and h == 1:
                send(x_takes | has_up, sa, yt, h, x_dev)
            if d and h == 0:
                send(x_takes & (c == 1), sa, yt, h, x_dev)
            send(exists, sa, yt, h, p_dev)

        def corner():
            wait(exists & has_up | x_gives, sb, yt, up_half)
            send(exists & has_up, sb, yt, up_half, up_dev)
            send(x_gives, sb, yt, up_half, p_dev)
            wait(x_gives, sb, yt, 1 - up_half)
            send(x_gives, sb, yt, 1 - up_half, p_dev)

        def transpose(sp):
            left[sp] = jnp.transpose(buf[sp, t])

        def product(sp, tp):
            lag = ((s - sp) * seg_days).astype(F32)
            gram = jnp.dot(left[sp], buf[sp, tp], preferred_element_type=F32)
            at = pl.ds(pl.multiple_of(tp * block, block), block)
            col, row = jnp.exp(-cols[...] * lag), jnp.exp(-rates_ref[:, at] * lag)
            for j in range(block // 128):
                lane = slice(j * 128, (j + 1) * 128)
                here = pl.ds(pl.multiple_of(tp * block + j * 128, 128), 128)
                out_ref[:, here] += gram[:, lane] * (col * row[:, lane])

        def products(first, last, which):
            def step(i, _):
                product(*which(i))
                return 0

            lax.fori_loop(first, last, step, 0)

        def column_products():
            @pl.when(exists)
            def _():
                for h in (0, 1):
                    arrived(sa, pt, h)
                transpose(sa)
                products(0, 2, lambda i: (sa, y * CORES + i))

        def across_products():
            for h in (0, 1):
                wait(x_gives, sb, pt, h)
                wait(exists, sa, pyt, h)

            @pl.when(x_gives)
            def _():
                transpose(sb)

            @pl.when(exists)
            def _():
                products(
                    jnp.where(x_gives, 0, 2),
                    4,
                    lambda i: (
                        jnp.where(i < 2, sb, sa),
                        jnp.where(i < 2, y * CORES + i, (1 - y) * CORES + i - 2),
                    ),
                )

        def corner_products():
            @pl.when(x_gives)
            def _():
                for h in (0, 1):
                    arrived(sb, pyt, h)
                products(0, 2, lambda i: (sb, (1 - y) * CORES + i))

        return column, across, corner, column_products, across_products, corner_products

    column, across, corner, column_products, across_products, corner_products = zip(
        *[plane(d) for d in range(planes)]
    )

    elapsed = ((s + 1) * seg_days).astype(F32)

    def weigh(first):
        u1, un = expm1_neg(-cols[...]), expm1_neg(-cols[...] * elapsed)

        def step(j, _):
            at = pl.ds(pl.multiple_of(first * block + j * 128, 128), 128)
            rates = rates_ref[:, at]
            v1, vn = expm1_neg(-rates), expm1_neg(-rates * elapsed)
            ratio[:, at] = (u1 + v1 + u1 * v1) / (un + vn + un * vn)
            return 0

        lax.fori_loop(0, CORES * block // 128, step, 0)

    def finish(first):
        at = pl.ds(pl.multiple_of(first * block, block), CORES * block)
        out_ref[:, at] = out_ref[:, at] * ratio[:, at]

    column[0](0)
    column[0](1)
    column_products[0]()
    weigh(y * CORES)
    for d in range(planes):
        more = d + 1 < planes
        if more:
            column[d + 1](0)
        if d:
            corner[d - 1]()
        across[d](0)
        if more:
            column[d + 1](1)
        across[d](1)
        if d:
            corner_products[d - 1]()
        if not more:
            corner[d]()
        across_products[d]()
        if d == 1:
            weigh((1 - y) * CORES)
        if more:
            column_products[d + 1]()
    finish(y * CORES)
    corner_products[-1]()
    finish((1 - y) * CORES)

    for cond, sp, tp, h, dev, sem in sent:

        @pl.when(cond)
        def _(sp=sp, tp=tp, h=h, dev=dev, sem=sem):
            copy(sp, tp, h, dev, sem).wait_send()


def by_gather(returns, decay_rates):
    seg_days, block = returns.shape
    periods, tiles = lax.axis_size("tm"), lax.axis_size("tile")
    assets = decay_rates.shape[0]
    planes = periods // (tiles // CORES)
    vmem = pl.BlockSpec(memory_space=pltpu.VMEM)
    return pl.pallas_call(
        functools.partial(gather_kernel, periods, tiles),
        out_shape=jax.ShapeDtypeStruct((block, assets), F32),
        in_specs=[vmem, vmem],
        out_specs=vmem,
        scratch_shapes=[
            pltpu.VMEM((periods, tiles, seg_days, block), jnp.bfloat16),
            pltpu.VMEM((periods, block, seg_days), jnp.bfloat16),
            pltpu.VMEM((block, assets), F32),
            pltpu.VMEM((block, 128), F32),
            pltpu.SemaphoreType.DMA((planes, 20)),
            pltpu.SemaphoreType.DMA((periods, tiles, 2)),
        ],
        compiler_params=pltpu.CompilerParams(
            collective_id=0, has_side_effects=True, vmem_limit_bytes=40 * 2**20
        ),
        name="gather_sums",
    )(returns, decay_rates[None])[None]


def by_exchange(returns, decay_rates):
    seg_days, col_block = returns.shape
    tile_at = lax.axis_index("tile")
    seg_at = lax.axis_index("tm")
    days_left = (seg_days - 1 - jnp.arange(seg_days)).astype(jnp.float32)
    own_rates = lax.dynamic_slice_in_dim(decay_rates, tile_at * col_block, col_block)
    scaled = (returns * jnp.exp(-own_rates[None, :] * days_left[:, None])).astype(jnp.bfloat16)
    gram_rows = lax.dot_general(
        scaled,
        lax.all_gather(scaled, "tile", axis=1, tiled=True),
        (((0,), (0,)), ((), ())),
        preferred_element_type=jnp.float32,
    )
    pair_rate = own_rates[:, None] + decay_rates[None, :]
    seg_decay = jnp.exp(-pair_rate * seg_days)
    periods = lax.axis_size("tm")
    row_piece = col_block // periods
    spread = lax.all_to_all(gram_rows[None], "tm", split_axis=1, concat_axis=0, tiled=True)
    row_rates = lax.dynamic_slice_in_dim(
        decay_rates, tile_at * col_block + seg_at * row_piece, row_piece
    )
    row_decay = jnp.exp(-(row_rates[:, None] + decay_rates[None, :]) * seg_days)

    def advance(running, segment_term):
        return (running * row_decay + segment_term, running)

    _, prefix = lax.scan(advance, jnp.zeros_like(spread[0]), spread)
    carried = lax.all_to_all(prefix, "tm", split_axis=0, concat_axis=1, tiled=True)[0]
    running = carried * seg_decay + gram_rows
    elapsed = (seg_at + 1).astype(jnp.float32) * seg_days
    weights = jnp.expm1(-pair_rate * elapsed) / jnp.expm1(-pair_rate)
    return (running / weights)[None]


def solution(mesh):
    placed = (P("tm", "tile"), P())
    pairs = mesh.shape["tile"] == 2 * CORES
    per_device = by_gather if pairs else by_exchange
    return jax.shard_map(
        per_device, mesh=mesh, in_specs=placed, out_specs=P("tm", "tile", None), check_vma=False
    )
```
